128 devices in a mesh: replica: 8 (over z, core), tp: 16 (over y, x).
Axes of the slice: x: 4, y: 4, z: 4, core: 2. Of those that a mesh axis runs over, the one named last changes fastest.
Arguments:
- hidden: bfloat16 [1024, 8192], P(('replica', 'tp')), may hold values from -64 to 64
- head: bfloat16 [152064, 8192], P(('replica', 'tp'))
- token_ids: int32 [1024], replicated, may hold values from 0 to 152063
Outputs:
- logprob: float32 [1024], P(('replica', 'tp'))
The draws below stay inside these ranges and needn't reach their ends.
All inputs are finite; a program needn't handle non-finite values.
Results may differ from the reference program's by a relative error of at most 0.0003.
Values may be sent and summed in bfloat16 or wider, within the bound.
A program may use at most 128 MiB of HBM per device.

```python
import math
import jax
import jax.numpy as jnp
from jax import lax

D = 8192
V = 152064
SEQS = 1024


def head_row(key, index):
    values = jax.random.normal(jax.random.fold_in(key, index), (D,), jnp.float32)
    return jnp.clip(values, -6.0, 6.0) * (3.0 / math.sqrt(D))


def head_rows(key, indices):
    base = jax.random.fold_in(key, 11)
    return jax.vmap(lambda index: head_row(base, index))(indices)


def draw_head(key, part):
    return head_rows(key, jnp.arange(V, dtype=jnp.int32)).astype(jnp.bfloat16)


def draw_hidden(key, part):
    drawn = jnp.clip(jax.random.normal(jax.random.fold_in(key, 21), (SEQS, D), jnp.float32), -6.0, 6.0)
    return drawn.astype(jnp.bfloat16)


def place_ends(result, rng, smallest, largest):
    index_at = [jax.random.randint(jax.random.fold_in(rng, axis), (), 0, length) for axis, length in enumerate(result.shape)]
    main_axis = result.shape.index(max(result.shape))
    beside = index_at[:main_axis] + [(index_at[main_axis] + 1) % result.shape[main_axis]] + index_at[main_axis + 1:]
    return result.at[tuple(index_at)].set(smallest).at[tuple(beside)].set(largest)


def setup_inputs(seed: int = 0) -> dict:
    key_list = jax.random.split(jax.random.key(seed), 4)
    return {
        "hidden": draw_hidden(jax.random.fold_in(key_list[3], 71), 0),
        "head": draw_head(jax.random.fold_in(key_list[3], 71), 0),
        "token_ids": place_ends(jax.random.randint(key_list[2], (SEQS,), 0, V), jax.random.fold_in(key_list[2], 1), 0, V - 1).astype(jnp.int32),
    }


def reference(hidden, head, token_ids):
    logits = lax.dot_general(hidden, head, (((1,), (1,)), ((), ())), preferred_element_type=jnp.float32)
    row_top = jnp.max(logits, axis=1)
    row_total = jnp.sum(jnp.exp(logits - row_top[:, None]), axis=1)
    row_picked = jnp.take_along_axis(logits, token_ids[:, None].astype(jnp.int32), axis=1)[:, 0]
    return row_picked - row_top - jnp.log(row_total)
```

```python
import functools

import jax
import jax.numpy as jnp
from jax import lax
from jax.experimental import pallas as pl
from jax.experimental.pallas import tpu as pltpu
from jax.sharding import PartitionSpec as P

MESH = pl.DeviceIdType.MESH
ROTATIONS = ((2, 1, 0), (1, 0, 2), (0, 2, 1))
UNIT = 256
WIDTHS = (11, 11, 10)
STAGE = 2
STAGES = 5
FIRST = (0, 11, 22)
ALL = (0, 4)


def at(rotation, e1, e2, e3):
    where = [None, None, None]
    for axis, e in zip(ROTATIONS[rotation], (e1, e2, e3)):
        where[axis] = pl.ds(e[0], e[1]) if isinstance(e, tuple) else e
    return tuple(where)


def kernel(hidden, head, ids, out, blocks, weights, logits, rolled, chip, chip_in, plane, plane_in,
           head_sem, own_sem, send_sem, recv_sem, loop_send, loop_recv):
    replica, tp = lax.axis_index("replica"), lax.axis_index("tp")
    z, core = replica // 2, lax.rem(replica, 2)
    y, x = tp // 4, lax.rem(tp, 4)
    vocab, depth = head.shape

    def device(dz, dy, dx, other_core):
        c = 1 - core if other_core else core
        return (lax.rem(z + dz, 4) * 2 + c, lax.rem(y + dy, 4) * 4 + lax.rem(x + dx, 4))

    def neighbour(axis, step):
        move = [0, 0, 0]
        move[axis] = step % 4
        return device(*move, False)

    sibling = device(0, 0, 0, True)

    own = pltpu.make_async_copy(hidden, blocks.at[0, 0, 0, 0], own_sem)
    own.start()
    loads = []
    for k in range(4):
        part = pl.ds(k * depth // 4, depth // 4)
        loads.append(pltpu.make_async_copy(head.at[:, part], weights.at[:, part], head_sem.at[k]))
        loads[-1].start()

    barrier = pltpu.get_barrier_semaphore()
    for axis in range(3):
        for step in (1, -1):
            pl.semaphore_signal(barrier, inc=1, device_id=neighbour(axis, step), device_id_type=MESH)
    pl.semaphore_signal(barrier, inc=1, device_id=sibling, device_id_type=MESH)
    pl.semaphore_wait(barrier, 7)
    own.wait()

    used = [0]
    started = []

    def copy(src, dst, target):
        k = used[0]
        used[0] += 1
        c = pltpu.make_async_remote_copy(
            src_ref=src, dst_ref=dst, send_sem=send_sem.at[k], recv_sem=recv_sem.at[k],
            device_id=target, device_id_type=MESH)
        c.start()
        started.append(c)
        return c

    def columns(r, first, count):
        return pl.ds((FIRST[r] + first) * UNIT, count * UNIT)

    def hop(r, which, step, src, dst, cols):
        return copy(blocks.at[(0,) + at(r, *src) + (slice(None), cols)],
                    blocks.at[(0,) + at(r, *dst) + (slice(None), cols)],
                    neighbour(ROTATIONS[r][which], step))

    def share(r, where, cols):
        return copy(blocks.at[(0,) + at(r, *where) + (slice(None), cols)],
                    blocks.at[(1,) + at(r, *where) + (slice(None), cols)], sibling)

    full = [columns(r, 0, WIDTHS[r]) for r in range(3)]
    RS = range(3)
    one_up = [hop(r, 0, 1, (0, 0, 0), (3, 0, 0), full[r]) for r in RS]
    one_down = [hop(r, 0, -1, (0, 0, 0), (1, 0, 0), full[r]) for r in RS]

    def second(r, e1):
        return (hop(r, 1, 1, (e1, 0, 0), (e1, 3, 0), full[r]), hop(r, 1, -1, (e1, 0, 0), (e1, 1, 0), full[r]))

    two = [[None] * 4 for _ in RS]
    for r in RS:
        two[r][0] = second(r, 0)

    logits[...] = jnp.zeros_like(logits)
    logits[pl.ds(vocab, 4), :] = jnp.full((4, logits.shape[1]), -3.0e38, jnp.float32)
    lane = lax.broadcasted_iota(jnp.int32, (8, 128), 1)
    turned = pltpu.roll(ids[...], lax.rem(128 - y * 32, 128), 1)
    near = pltpu.roll(turned, lax.rem(128 - x * 8, 128), 1)
    far = pltpu.roll(turned, lax.rem(160 - x * 8, 128), 1)
    turned = jnp.where(lax.rem(lane, 32) + x * 8 < 32, near, far) - (replica * 16 + tp) * vocab
    rolled[...] = jnp.where((turned >= 0) & (turned < vocab), turned, -1)

    one_far = []
    for r in RS:
        half = (WIDTHS[r] + 1) // 2
        one_up[r].wait_recv()
        a = hop(r, 0, 1, (3, 0, 0), (2, 0, 0), columns(r, 0, half))
        two[r][3] = second(r, 3)
        one_down[r].wait_recv()
        b = hop(r, 0, -1, (1, 0, 0), (2, 0, 0), columns(r, half, WIDTHS[r] - half))
        two[r][1] = second(r, 1)
        one_far.append((a, b))

    three = []
    two_far = [[None] * 4 for _ in RS]
    for r in RS:
        for c in one_far[r]:
            c.wait_recv()
        two[r][2] = second(r, 2)
        three.append((hop(r, 2, 1, (ALL, 0, 0), (ALL, 0, 3), full[r]), hop(r, 2, -1, (ALL, 0, 0), (ALL, 0, 1), full[r])))

    def onward(r, e1):
        up, down = two[r][e1]
        up.wait_recv()
        down.wait_recv()
        if e1 < 2:
            two_far[r][e1] = hop(r, 1, 1, (e1, 3, 0), (e1, 2, 0), full[r])
        else:
            two_far[r][e1] = hop(r, 1, -1, (e1, 1, 0), (e1, 2, 0), full[r])

    for e1 in (0, 1, 3, 2):
        for r in RS:
            onward(r, e1)

    REST = (1, 3)

    def loop_cols(r, s):
        return pl.ds(pl.multiple_of((FIRST[r] + s * STAGE) * UNIT, UNIT), STAGE * UNIT)

    def loop_copy(s, r, kind):
        cols = loop_cols(r, s)
        src, dst, which, step = (
            ((ALL, REST, 0), (ALL, REST, 3), 2, 1),
            ((ALL, REST, 0), (ALL, REST, 1), 2, -1),
            (((0, 2), REST, 3), ((0, 2), REST, 2), 2, 1),
            (((2, 2), REST, 1), ((2, 2), REST, 2), 2, -1),
            ((ALL, REST, (1, 3)), (ALL, REST, (1, 3)), None, None),
        )[kind]
        target = sibling if which is None else neighbour(ROTATIONS[r][which], step)
        return pltpu.make_async_remote_copy(
            src_ref=blocks.at[(0,) + at(r, *src) + (slice(None), cols)],
            dst_ref=blocks.at[(1 if which is None else 0,) + at(r, *dst) + (slice(None), cols)],
            send_sem=loop_send.at[s, r * 5 + kind], recv_sem=loop_recv.at[s, r * 5 + kind],
            device_id=target, device_id_type=MESH)

    shares = []
    for r in RS:
        for c in two_far[r]:
            c.wait_recv()
        for s in range(1):
            loop_copy(s, r, 0).start()
            loop_copy(s, r, 1).start()
        shares.append(share(r, (ALL, ALL, 0), full[r]))

    three_far = []
    for r in RS:
        three[r][0].wait_recv()
        a = hop(r, 2, 1, ((0, 2), 0, 3), ((0, 2), 0, 2), full[r])
        three[r][1].wait_recv()
        b = hop(r, 2, -1, ((2, 2), 0, 1), ((2, 2), 0, 2), full[r])
        three_far.append((a, b))
        loop_copy(1, r, 0).start()
        loop_copy(1, r, 1).start()

    tail = []
    for r in (0, 1):
        cols = columns(r, STAGE * STAGES, 1)
        tail.append((hop(r, 2, 1, (ALL, REST, 0), (ALL, REST, 3), cols), hop(r, 2, -1, (ALL, REST, 0), (ALL, REST, 1), cols)))
    for r in RS:
        for c in three_far[r]:
            c.wait_recv()
        shares.append(share(r, (ALL, 0, (1, 3)), full[r]))
    for c in loads:
        c.wait()

    half_lanes = logits.shape[1] // 2

    def multiply(side, cols):
        a = jnp.concatenate([weights[:, c] for c in cols], axis=1)
        b = jnp.concatenate([blocks[side, :, :, :, :, c].reshape(half_lanes, c.size) for c in cols], axis=1)
        product = lax.dot_general(a, b, (((1,), (1,)), ((), ())), preferred_element_type=jnp.float32)
        where = (pl.ds(0, vocab), pl.ds(side * half_lanes, half_lanes))
        logits[where] = logits[where] + product

    def arrive(s):
        for r in RS:
            loop_copy(s, r, 0).wait_recv()
            loop_copy(s, r, 2).start()
            loop_copy(s, r, 1).wait_recv()
            loop_copy(s, r, 3).start()

    def finish(s):
        for r in RS:
            loop_copy(s, r, 2).wait_recv()
            loop_copy(s, r, 3).wait_recv()
            loop_copy(s, r, 4).start()

    def stage_cols(s):
        return [loop_cols(r, s) for r in RS]

    def queue(s):
        for r in RS:
            loop_copy(s, r, 0).start()
            loop_copy(s, r, 1).start()

    arrive(0)
    queue(2)
    finish(0)
    multiply(0, stage_cols(0))
    for c in shares:
        c.wait_recv()

    def stage(s, _):
        arrive(s)

        @pl.when(s + 2 < STAGES)
        def _():
            queue(s + 2)

        for r in RS:
            loop_copy(s - 1, r, 4).wait_recv()
        multiply(1, stage_cols(s - 1))
        finish(s)
        multiply(0, stage_cols(s))
        return 0

    lax.fori_loop(1, STAGES, stage, 0)

    tail_cols = [columns(r, STAGE * STAGES, 1) for r in (0, 1)]
    tail_far = []
    for r in (0, 1):
        tail[r][0].wait_recv()
        a = hop(r, 2, 1, ((0, 2), REST, 3), ((0, 2), REST, 2), tail_cols[r])
        tail[r][1].wait_recv()
        b = hop(r, 2, -1, ((2, 2), REST, 1), ((2, 2), REST, 2), tail_cols[r])
        tail_far.append((a, b))
    for r in RS:
        loop_copy(STAGES - 1, r, 4).wait_recv()
    multiply(1, stage_cols(STAGES - 1))
    tail_share = []
    for r in (0, 1):
        for c in tail_far[r]:
            c.wait_recv()
        tail_share.append(share(r, (ALL, REST, (1, 3)), tail_cols[r]))
    multiply(0, tail_cols)
    for c in tail_share:
        c.wait_recv()
    multiply(1, tail_cols)

    lanes = logits.shape[1]
    rows = 32
    count = logits.shape[0] // rows
    left = logits.shape[0] - rows * count

    def groups(value):
        return [value[8 * k:8 * k + 8, :] for k in range(value.shape[0] // 8)]

    def top_step(i, top):
        for v in groups(logits[pl.ds(pl.multiple_of(i * rows, rows), rows), :]):
            top = jnp.maximum(top, v)
        return top

    top = lax.fori_loop(0, count, top_step, logits[pl.ds(rows * count, left), :])
    top = jnp.max(top, axis=0, keepdims=True)

    order = [(c, dz) for c in range(2) for dz in range(4)]
    wanted = jnp.concatenate(
        [rolled[pl.ds(lax.rem(z + dz, 4) * 2 + (1 - core if c else core), 1), :] for c, dz in order], axis=1)
    row = lax.broadcasted_iota(jnp.int32, (8, lanes), 0)
    offset = jnp.broadcast_to(wanted, (8, lanes)) - row

    def add(v, first, total, picked):
        total = total + jnp.exp(v - top)
        picked = picked + jnp.where(offset == first, v, 0.0)
        return total, picked

    def sum_step(i, carry):
        total, picked = carry
        for k, v in enumerate(groups(logits[pl.ds(pl.multiple_of(i * rows, rows), rows), :])):
            total, picked = add(v, i * rows + 8 * k, total, picked)
        return total, picked

    zero = jnp.zeros((8, lanes), jnp.float32)
    total, picked = lax.fori_loop(0, count, sum_step, (zero, zero))
    total, picked = add(logits[pl.ds(rows * count, left), :], rows * count, total, picked)
    total = jnp.sum(total, axis=0, keepdims=True)
    picked = jnp.sum(picked, axis=0, keepdims=True)

    for k in range(8):
        part = slice(128 * k, 128 * k + 128)
        chip[k, 0:1, :] = top[:, part]
        chip[k, 1:2, :] = total[:, part]
        chip[k, 2:3, :] = picked[:, part]
    ups = []
    for k, (c, dz) in enumerate(order):
        if k:
            ups.append(copy(chip.at[k], chip_in.at[c * 4 + (-dz) % 4], device(dz, 0, 0, c)))
    for c in ups:
        c.wait_recv()

    def merge(parts):
        best = functools.reduce(jnp.maximum, [p[0] for p in parts])
        total = sum(p[1] * jnp.exp(p[0] - best) for p in parts)
        return best, total, sum(p[2] for p in parts)

    def three_rows(ref, *at):
        return tuple(ref[at + (pl.ds(k, 1), slice(None))] for k in range(3))

    best, total, picked = merge([three_rows(chip, 0)] + [three_rows(chip_in, k) for k in range(1, 8)])
    plane[0:1, :] = best
    plane[1:2, :] = total
    plane[2:3, :] = picked
    across = []
    for dy in range(4):
        for dx in range(4):
            if dy or dx:
                across.append(copy(plane, plane_in.at[(-dy) % 4 * 4 + (-dx) % 4], device(0, dy, dx, False)))
    for c in across:
        c.wait_recv()
    group = lax.broadcasted_iota(jnp.int32, (1, 128), 1) // 8
    for sy in range(4):
        for sx in range(4):
            if sy or sx:
                mine = group == (-sy) % 4 * 4 + (-sx) % 4
                b, t, p = three_rows(plane_in, sy * 4 + sx)
                best, total, picked = jnp.where(mine, b, best), jnp.where(mine, t, total), jnp.where(mine, p, picked)
    final = best
    for shift in (8, 16, 32, 64):
        final = jnp.maximum(final, pltpu.roll(final, shift, 1))
    total = total * jnp.exp(best - final)
    for shift in (8, 16, 32, 64):
        total = total + pltpu.roll(total, shift, 1)
        picked = picked + pltpu.roll(picked, shift, 1)
    out[...] = picked - final - jnp.log(total)

    for c in started:
        c.wait_send()

    def drain(s, _):
        for r in RS:
            for kind in range(5):
                loop_copy(s, r, kind).wait_send()
        return 0

    lax.fori_loop(0, STAGES, drain, 0)


COPIES = 150


def shards(hidden, head, token_ids):
    vocab, depth = head.shape
    lanes = token_ids.shape[0]
    out = pl.pallas_call(
        kernel,
        out_shape=jax.ShapeDtypeStruct((1, 128), jnp.float32),
        in_specs=[pl.BlockSpec(memory_space=pl.ANY), pl.BlockSpec(memory_space=pl.ANY),
                  pl.BlockSpec(memory_space=pltpu.VMEM)],
        out_specs=pl.BlockSpec(memory_space=pltpu.VMEM),
        scratch_shapes=[
            pltpu.VMEM((2, 4, 4, 4, 8, depth), jnp.bfloat16),
            pltpu.VMEM((vocab, depth), jnp.bfloat16),
            pltpu.VMEM((vocab + 4, lanes), jnp.float32),
            pltpu.VMEM((8, 128), jnp.int32),
            pltpu.VMEM((8, 8, 128), jnp.float32),
            pltpu.VMEM((8, 8, 128), jnp.float32),
            pltpu.VMEM((8, 128), jnp.float32),
            pltpu.VMEM((16, 8, 128), jnp.float32),
            pltpu.SemaphoreType.DMA((4,)),
            pltpu.SemaphoreType.DMA,
            pltpu.SemaphoreType.DMA((COPIES,)),
            pltpu.SemaphoreType.DMA((COPIES,)),
            pltpu.SemaphoreType.DMA((STAGES, 15)),
            pltpu.SemaphoreType.DMA((STAGES, 15)),
        ],
        compiler_params=pltpu.CompilerParams(
            collective_id=0, has_side_effects=True, vmem_limit_bytes=60 * 1024 * 1024),
        name="logprob",
    )(hidden, head, token_ids.reshape(8, 128))
    return out[0, :8]


def solution(mesh):
    in_specs = (P(("replica", "tp"), None), P(("replica", "tp"), None), P())
    out_specs = P(("replica", "tp"))
    return jax.shard_map(shards, mesh=mesh, in_specs=in_specs, out_specs=out_specs, check_vma=False)
```

```python
import functools

import jax
import jax.numpy as jnp
from jax import lax
from jax.experimental import pallas as pl
from jax.experimental.pallas import tpu as pltpu
from jax.sharding import PartitionSpec as P

MESH = pl.DeviceIdType.MESH
ROTATIONS = ((2, 1, 0), (1, 0, 2), (0, 2, 1))
UNIT = 256
FIRST = (0, 11, 22)
TOTAL = (11, 11, 10)
STAGES = ((1, 1, 1), (1, 1, 1), (2, 2, 2), (2, 2, 2), (2, 2, 2), (2, 2, 2), (1, 1, 0))
WHOLE = (0, 1, 6)
PASSED = (3, 4, 5, 6)
FINAL = (3, 3)
ORDER = (
    "S0", "rest", "S5", "load", "S4", "S2", "T0", "G5", "G4", "S6", "T2", "A0",
    "S3", "T4", "M0", "G6", "A2", "G3", "T5", "A4", "N0", "S1", "F2", "T3",
    "M2", "A5", "N2", "T6", "T1", "F4", "M4", "N4", "F5", "A3", "M5", "A6",
    "N5", "M6", "A1", "N6", "M1", "F3", "M3", "N1", "N3",
)
START = tuple(tuple(FIRST[r] + sum(st[r] for st in STAGES[:k]) for r in range(3)) for k in range(len(STAGES)))
ALL, NEAR = (0, 4), (0, 3)
KINDS = 6
SECOND, PASS, DIRECT, FORWARD, SHARE, SHARE_FAR = range(KINDS)
LATE = KINDS * len(STAGES)
ONE, ONE_REST, CHIP, PLANE = range(LATE, LATE + 4)


def at(rotation, e1, e2, e3):
    where = [None, None, None]
    for axis, e in zip(ROTATIONS[rotation], (e1, e2, e3)):
        where[axis] = pl.ds(e[0], e[1]) if isinstance(e, tuple) else e
    return tuple(where)


def region(count):
    for units in range(32, 0, -1):
        if count % units:
            continue
        for c in (1, 2):
            for i in range(1, 5):
                for j in range(1, 5):
                    for k in range(1, 5):
                        if c * i * j * k * units == count:
                            return (pl.ds(0, c), pl.ds(0, i), pl.ds(0, j), pl.ds(0, k), slice(None), pl.ds(0, units * UNIT))
    raise ValueError(count)


def kernel(hidden, head, token_ids, out, blocks, weights, logits, ids, rolled, chip, chip_in, plane, plane_in,
           head_sem, own_sem, ids_sem, send_sem, recv_sem):
    replica, tp = lax.axis_index("replica"), lax.axis_index("tp")
    z, core = replica // 2, lax.rem(replica, 2)
    y, x = tp // 4, lax.rem(tp, 4)
    vocab, depth = head.shape
    RS = range(3)

    def device(dz, dy, dx, other_core):
        c = 1 - core if other_core else core
        return (lax.rem(z + dz, 4) * 2 + c, lax.rem(y + dy, 4) * 4 + lax.rem(x + dx, 4))

    def neighbour(axis, step):
        move = [0, 0, 0]
        move[axis] = step % 4
        return device(*move, False)

    sibling = device(0, 0, 0, True)

    own = pltpu.make_async_copy(hidden, blocks.at[0, 1, 1, 1], own_sem)
    own.start()
    fetch = pltpu.make_async_copy(token_ids, ids, ids_sem)
    fetch.start()
    load = pltpu.make_async_copy(head, weights, head_sem)
    load.start()

    barrier = pltpu.get_barrier_semaphore()
    for axis in range(3):
        for step in (1, -1, 2):
            pl.semaphore_signal(barrier, inc=1, device_id=neighbour(axis, step), device_id_type=MESH)
    pl.semaphore_signal(barrier, inc=1, device_id=sibling, device_id_type=MESH)
    pl.semaphore_wait(barrier, 10)
    own.wait()

    sent = {}

    def kind(group):
        return group % KINDS if group < LATE else KINDS + group - LATE

    def remote(src, dst, target, group):
        return pltpu.make_async_remote_copy(
            src_ref=src, dst_ref=dst, send_sem=send_sem.at[kind(group)], recv_sem=recv_sem.at[group],
            device_id=target, device_id_type=MESH)

    def move(r, src, dst, cols, target, group, side=0):
        a = at(r, *src)
        remote(blocks.at[(0,) + a + (slice(None), cols)],
               blocks.at[(side,) + at(r, *dst) + (slice(None), cols)], target, group).start()
        size = cols.size // UNIT
        for e in src:
            size *= e[1] if isinstance(e, tuple) else 1
        sent[group] = sent.get(group, 0) + size

    def arrived(group):
        where = blocks.at[region(sent[group])]
        remote(where, where, sibling, group).wait_recv()

    def drained():
        totals = {}
        for group, count in sent.items():
            totals[kind(group)] = totals.get(kind(group), 0) + count
        for k, count in totals.items():
            where = blocks.at[region(count)]
            pltpu.make_async_remote_copy(
                src_ref=where, dst_ref=where, send_sem=send_sem.at[k], recv_sem=recv_sem.at[0],
                device_id=sibling, device_id_type=MESH).wait_send()

    def cols_of(k, r):
        return pl.ds(START[k][r] * UNIT, STAGES[k][r] * UNIT)

    def ring(r, which, src, dst, cols, group, steps):
        for step in steps:
            to = list(dst)
            to[which] = (1 - step) % 4
            move(r, src, tuple(to), cols, neighbour(ROTATIONS[r][which], step), group)

    def live(k):
        return [r for r in RS if STAGES[k][r]]

    def second(k):
        for step in (1, -1) if k in PASSED else (1, -1, 2):
            for r in live(k):
                ring(r, 1, (ALL, 1, 1), (ALL, 1, 1), cols_of(k, r), k * KINDS + SECOND, (step,))

    def onward(k):
        arrived(k * KINDS + SECOND)
        for r in live(k):
            move(r, ((0, 2), 0, 1), ((0, 2), 3, 1), cols_of(k, r), neighbour(ROTATIONS[r][1], 1), k * KINDS + PASS)
            move(r, ((2, 2), 2, 1), ((2, 2), 3, 1), cols_of(k, r), neighbour(ROTATIONS[r][1], -1), k * KINDS + PASS)

    def third(k):
        arrived(k * KINDS + (PASS if k in PASSED else SECOND))
        for step in (1, -1, 2) if k in WHOLE else (1, -1):
            for r in live(k):
                ring(r, 2, (ALL, ALL, 1), (ALL, ALL, 1), cols_of(k, r), k * KINDS + DIRECT, (step,))

    def arrive(k):
        arrived(k * KINDS + DIRECT)
        for r in live(k):
            if k not in WHOLE:
                move(r, ((0, 2), ALL, 0), ((0, 2), ALL, 3), cols_of(k, r), neighbour(ROTATIONS[r][2], 1), k * KINDS + FORWARD)
                move(r, ((2, 2), ALL, 2), ((2, 2), ALL, 3), cols_of(k, r), neighbour(ROTATIONS[r][2], -1), k * KINDS + FORWARD)
        for r in live(k):
            part = ALL if k in WHOLE else NEAR
            move(r, (ALL, ALL, part), (ALL, ALL, part), cols_of(k, r), sibling, k * KINDS + SHARE, 1)

    def finish(k):
        arrived(k * KINDS + FORWARD)
        for r in live(k):
            move(r, (ALL, ALL, 3), (ALL, ALL, 3), cols_of(k, r), sibling, k * KINDS + SHARE_FAR, 1)

    def shared(k):
        arrived(k * KINDS + SHARE)
        if k not in WHOLE:
            arrived(k * KINDS + SHARE_FAR)

    half_lanes = logits.shape[1] // 2

    tops, tallies = {}, {}
    order = [(c, sz) for c in range(2) for sz in range(4)]

    def tally(side):
        top = jnp.broadcast_to(tops[side], (8, half_lanes))
        wanted = jnp.concatenate(
            [rolled[pl.ds(lax.rem(z + sz + 3, 4) * 2 + (1 - core if c else core), 1), :]
             for c, sz in order if c == side], axis=1)
        row = lax.broadcasted_iota(jnp.int32, (8, half_lanes), 0)
        offset = jnp.broadcast_to(wanted, (8, half_lanes)) - row
        total = picked = jnp.zeros((8, half_lanes), jnp.float32)
        for first in range(0, logits.shape[0], 8):
            v = logits[pl.ds(first, 8), pl.ds(side * half_lanes, half_lanes)]
            total = total + jnp.exp(v - top)
            picked = picked + jnp.where(offset == first, v, 0.0)
        return jnp.sum(total, axis=0, keepdims=True), jnp.sum(picked, axis=0, keepdims=True)

    def multiply(side, k):
        cols = [cols_of(k, r) for r in live(k)]
        a = jnp.concatenate([weights[:, c] for c in cols], axis=1)
        b = jnp.concatenate([blocks[side, :, :, :, :, c].reshape(half_lanes, c.size) for c in cols], axis=1)
        product = lax.dot_general(a, b, (((1,), (1,)), ((), ())), preferred_element_type=jnp.float32)
        where = (pl.ds(0, vocab), pl.ds(side * half_lanes, half_lanes))
        if k == 0:
            logits[where] = product
        else:
            product = logits[where] + product
            logits[where] = product
        if k == FINAL[side]:
            tops[side] = jnp.max(product, axis=0, keepdims=True)

    for step in (1, -1, 2):
        for r in RS:
            ring(r, 0, (1, 1, 1), (1, 1, 1), cols_of(0, r), ONE, (step,))
    for step in (1, -1, 2):
        for r in RS:
            rest = pl.ds(START[1][r] * UNIT, (TOTAL[r] - STAGES[0][r]) * UNIT)
            ring(r, 0, (1, 1, 1), (1, 1, 1), rest, ONE_REST, (step,))

    logits[pl.ds(vocab, 4), :] = jnp.full((4, logits.shape[1]), -jnp.inf, jnp.float32)
    fetch.wait()
    lane = lax.broadcasted_iota(jnp.int32, (8, 128), 1)
    y0, x0 = lax.rem(y + 3, 4), lax.rem(x + 3, 4)
    turned = pltpu.roll(ids[...], lax.rem(128 - y0 * 32, 128), 1)
    near = pltpu.roll(turned, lax.rem(128 - x0 * 8, 128), 1)
    far = pltpu.roll(turned, lax.rem(160 - x0 * 8, 128), 1)
    turned = jnp.where(lax.rem(lane, 32) + x0 * 8 < 32, near, far) - (replica * 16 + tp) * vocab
    rolled[...] = jnp.where((turned >= 0) & (turned < vocab), turned, -1)

    def other(k):
        shared(k)
        multiply(1, k)
        if k == FINAL[1]:
            tallies[0] = tally(0)

    def rest():
        arrived(ONE_REST)

    def loaded():
        load.wait()

    steps = {"S": second, "G": onward, "T": third, "A": arrive, "F": finish, "M": lambda k: multiply(0, k), "N": other}
    arrived(ONE)
    for step in ORDER:
        if step == "rest":
            arrived(ONE_REST)
        elif step == "load":
            load.wait()
        else:
            steps[step[0]](int(step[1:]))

    tallies[1] = tally(1)
    top, total, picked = [
        jnp.concatenate(both, axis=1)
        for both in ((tops[0], tops[1]), (tallies[0][0], tallies[1][0]), (tallies[0][1], tallies[1][1]))]

    for k in range(8):
        part = slice(128 * k, 128 * k + 128)
        chip[k, 0:1, :] = top[:, part]
        chip[k, 1:2, :] = total[:, part]
        chip[k, 2:3, :] = picked[:, part]
    for k, (c, sz) in enumerate(order):
        dz = (sz - 1) % 4
        if c or dz:
            remote(chip.at[k], chip_in.at[c * 4 + (-dz) % 4], device(dz, 0, 0, c), CHIP).start()
    remote(chip_in.at[pl.ds(1, 7)], chip_in.at[pl.ds(1, 7)], sibling, CHIP).wait_recv()

    def merge(parts):
        best = functools.reduce(jnp.maximum, [p[0] for p in parts])
        total = sum(p[1] * jnp.exp(p[0] - best) for p in parts)
        return best, total, sum(p[2] for p in parts)

    def three_rows(ref, *at):
        return tuple(ref[at + (pl.ds(k, 1), slice(None))] for k in range(3))

    best, total, picked = merge([three_rows(chip, 1)] + [three_rows(chip_in, k) for k in range(1, 8)])
    plane[0:1, :] = best
    plane[1:2, :] = total
    plane[2:3, :] = picked
    for dy in range(4):
        for dx in range(4):
            if dy or dx:
                remote(plane, plane_in.at[(-dy) % 4 * 4 + (-dx) % 4], device(0, dy, dx, False), PLANE).start()
    remote(plane_in.at[pl.ds(1, 15)], plane_in.at[pl.ds(1, 15)], sibling, PLANE).wait_recv()
    group = lax.broadcasted_iota(jnp.int32, (1, 128), 1) // 8
    for sy in range(4):
        for sx in range(4):
            if sy or sx:
                mine = group == (1 - sy) % 4 * 4 + (1 - sx) % 4
                b, t, p = three_rows(plane_in, sy * 4 + sx)
                best, total, picked = jnp.where(mine, b, best), jnp.where(mine, t, total), jnp.where(mine, p, picked)
    final = best
    for shift in (8, 16, 32, 64):
        final = jnp.maximum(final, pltpu.roll(final, shift, 1))
    total = total * jnp.exp(best - final)
    for shift in (8, 16, 32, 64):
        total = total + pltpu.roll(total, shift, 1)
        picked = picked + pltpu.roll(picked, shift, 1)
    out[...] = (picked - final - jnp.log(total))[:, :8]

    drained()
    remote(chip_in.at[pl.ds(1, 7)], chip_in.at[pl.ds(1, 7)], sibling, CHIP).wait_send()
    remote(plane_in.at[pl.ds(1, 15)], plane_in.at[pl.ds(1, 15)], sibling, PLANE).wait_send()


def shards(hidden, head, token_ids):
    vocab, depth = head.shape
    lanes = token_ids.shape[0]
    out = pl.pallas_call(
        kernel,
        out_shape=jax.ShapeDtypeStruct((1, 8), jnp.float32),
        in_specs=[pl.BlockSpec(memory_space=pl.ANY)] * 3,
        out_specs=pl.BlockSpec(memory_space=pltpu.VMEM),
        scratch_shapes=[
            pltpu.VMEM((2, 4, 4, 4, 8, depth), jnp.bfloat16),
            pltpu.VMEM((vocab, depth), jnp.bfloat16),
            pltpu.VMEM((vocab + 4, lanes), jnp.float32),
            pltpu.VMEM((8, 128), jnp.int32),
            pltpu.VMEM((8, 128), jnp.int32),
            pltpu.VMEM((8, 8, 128), jnp.float32),
            pltpu.VMEM((8, 8, 128), jnp.float32),
            pltpu.VMEM((8, 128), jnp.float32),
            pltpu.VMEM((16, 8, 128), jnp.float32),
            pltpu.SemaphoreType.DMA,
            pltpu.SemaphoreType.DMA,
            pltpu.SemaphoreType.DMA,
            pltpu.SemaphoreType.DMA((KINDS + 4,)),
            pltpu.SemaphoreType.DMA((LATE + 4,)),
        ],
        compiler_params=pltpu.CompilerParams(
            collective_id=0, has_side_effects=True, vmem_limit_bytes=60 * 1024 * 1024),
        name="logprob",
    )(hidden, head, token_ids.reshape(8, 128))
    return out.reshape(8)


def solution(mesh):
    in_specs = (P(("replica", "tp"), None), P(("replica", "tp"), None), P())
    out_specs = P(("replica", "tp"))
    return jax.shard_map(shards, mesh=mesh, in_specs=in_specs, out_specs=out_specs, check_vma=False)
```

```python
import functools

import jax
import jax.numpy as jnp
from jax import lax
from jax.experimental import pallas as pl
from jax.experimental.pallas import tpu as pltpu
from jax.sharding import PartitionSpec as P

MESH = pl.DeviceIdType.MESH
ROTATIONS = ((2, 1, 0), (1, 0, 2), (0, 2, 1))
UNIT = 256
FIRST = (0, 11, 22)
TOTAL = (11, 11, 10)
STAGES = ((1, 1, 1), (1, 1, 1), (2, 2, 2), (2, 2, 2), (2, 2, 2), (2, 2, 2), (1, 1, 0))
WHOLE = (0, 1, 6)
PASSED = (3, 4, 5, 6)
FINAL = (3, 3)
ORDER = (
    "S0", "rest", "S5", "load", "S4", "S2", "T0", "G5", "G4", "S6", "T2", "A0",
    "S3", "T4", "M0", "G6", "A2", "G3", "T5", "A4", "N0", "S1", "F2", "T3",
    "M2", "A5", "N2", "T6", "T1", "F4", "M4", "N4", "F5", "A3", "M5", "A6",
    "N5", "M6", "A1", "N6", "M1", "F3", "M3", "N1", "N3",
)
START = tuple(tuple(FIRST[r] + sum(st[r] for st in STAGES[:k]) for r in range(3)) for k in range(len(STAGES)))
ALL, NEAR = (0, 4), (0, 3)
KINDS = 6
SECOND, PASS, DIRECT, FORWARD, SHARE, SHARE_FAR = range(KINDS)
LATE = KINDS * len(STAGES)
ONE, ONE_REST, CHIP, PLANE = range(LATE, LATE + 4)


def at(rotation, e1, e2, e3):
    where = [None, None, None]
    for axis, e in zip(ROTATIONS[rotation], (e1, e2, e3)):
        where[axis] = pl.ds(e[0], e[1]) if isinstance(e, tuple) else e
    return tuple(where)


def region(count):
    for units in range(32, 0, -1):
        if count % units:
            continue
        for c in (1, 2):
            for i in range(1, 5):
                for j in range(1, 5):
                    for k in range(1, 5):
                        if c * i * j * k * units == count:
                            return (pl.ds(0, c), pl.ds(0, i), pl.ds(0, j), pl.ds(0, k), slice(None), pl.ds(0, units * UNIT))
    raise ValueError(count)


def kernel(hidden, head, token_ids, out, blocks, weights, logits, ids, rolled, chip, chip_in, plane, plane_in,
           head_sem, own_sem, ids_sem, send_sem, recv_sem):
    replica, tp = lax.axis_index("replica"), lax.axis_index("tp")
    z, core = replica // 2, lax.rem(replica, 2)
    y, x = tp // 4, lax.rem(tp, 4)
    vocab, depth = head.shape
    RS = range(3)

    def device(dz, dy, dx, other_core):
        c = 1 - core if other_core else core
        return (lax.rem(z + dz, 4) * 2 + c, lax.rem(y + dy, 4) * 4 + lax.rem(x + dx, 4))

    def neighbour(axis, step):
        move = [0, 0, 0]
        move[axis] = step % 4
        return device(*move, False)

    sibling = device(0, 0, 0, True)

    own = pltpu.make_async_copy(hidden, blocks.at[0, 1, 1, 1], own_sem)
    own.start()
    fetch = pltpu.make_async_copy(token_ids, ids, ids_sem)
    fetch.start()
    load = pltpu.make_async_copy(head, weights, head_sem)
    load.start()

    barrier = pltpu.get_barrier_semaphore()
    for axis in range(3):
        for step in (1, -1, 2):
            pl.semaphore_signal(barrier, inc=1, device_id=neighbour(axis, step), device_id_type=MESH)
    pl.semaphore_signal(barrier, inc=1, device_id=sibling, device_id_type=MESH)
    pl.semaphore_wait(barrier, 10)
    own.wait()

    sent = {}

    def kind(group):
        return group % KINDS if group < LATE else KINDS + group - LATE

    def remote(src, dst, target, group):
        return pltpu.make_async_remote_copy(
            src_ref=src, dst_ref=dst, send_sem=send_sem.at[kind(group)], recv_sem=recv_sem.at[group],
            device_id=target, device_id_type=MESH)

    def move(r, src, dst, cols, target, group, side=0):
        a = at(r, *src)
        remote(blocks.at[(0,) + a + (slice(None), cols)],
               blocks.at[(side,) + at(r, *dst) + (slice(None), cols)], target, group).start()
        size = cols.size // UNIT
        for e in src:
            size *= e[1] if isinstance(e, tuple) else 1
        sent[group] = sent.get(group, 0) + size

    def arrived(group):
        where = blocks.at[region(sent[group])]
        remote(where, where, sibling, group).wait_recv()

    def drained():
        totals = {}
        for group, count in sent.items():
            totals[kind(group)] = totals.get(kind(group), 0) + count
        for k, count in totals.items():
            where = blocks.at[region(count)]
            pltpu.make_async_remote_copy(
                src_ref=where, dst_ref=where, send_sem=send_sem.at[k], recv_sem=recv_sem.at[0],
                device_id=sibling, device_id_type=MESH).wait_send()

    def cols_of(k, r):
        return pl.ds(START[k][r] * UNIT, STAGES[k][r] * UNIT)

    def ring(r, which, src, dst, cols, group, steps):
        for step in steps:
            to = list(dst)
            to[which] = (1 - step) % 4
            move(r, src, tuple(to), cols, neighbour(ROTATIONS[r][which], step), group)

    def live(k):
        return [r for r in RS if STAGES[k][r]]

    def second(k):
        for r in live(k):
            for step in (1, -1) if k in PASSED else (1, -1, 2):
                ring(r, 1, (ALL, 1, 1), (ALL, 1, 1), cols_of(k, r), k * KINDS + SECOND, (step,))

    def onward(k):
        arrived(k * KINDS + SECOND)
        for r in live(k):
            move(r, ((0, 2), 0, 1), ((0, 2), 3, 1), cols_of(k, r), neighbour(ROTATIONS[r][1], 1), k * KINDS + PASS)
            move(r, ((2, 2), 2, 1), ((2, 2), 3, 1), cols_of(k, r), neighbour(ROTATIONS[r][1], -1), k * KINDS + PASS)

    def third(k):
        arrived(k * KINDS + (PASS if k in PASSED else SECOND))
        for r in live(k):
            for step in (1, -1, 2) if k in WHOLE else (1, -1):
                ring(r, 2, (ALL, ALL, 1), (ALL, ALL, 1), cols_of(k, r), k * KINDS + DIRECT, (step,))

    def arrive(k):
        arrived(k * KINDS + DIRECT)
        for r in live(k):
            if k not in WHOLE:
                move(r, ((0, 2), ALL, 0), ((0, 2), ALL, 3), cols_of(k, r), neighbour(ROTATIONS[r][2], 1), k * KINDS + FORWARD)
                move(r, ((2, 2), ALL, 2), ((2, 2), ALL, 3), cols_of(k, r), neighbour(ROTATIONS[r][2], -1), k * KINDS + FORWARD)
        for r in live(k):
            part = ALL if k in WHOLE else NEAR
            move(r, (ALL, ALL, part), (ALL, ALL, part), cols_of(k, r), sibling, k * KINDS + SHARE, 1)

    def finish(k):
        arrived(k * KINDS + FORWARD)
        for r in live(k):
            move(r, (ALL, ALL, 3), (ALL, ALL, 3), cols_of(k, r), sibling, k * KINDS + SHARE_FAR, 1)

    def shared(k):
        arrived(k * KINDS + SHARE)
        if k not in WHOLE:
            arrived(k * KINDS + SHARE_FAR)

    half_lanes = logits.shape[1] // 2

    tops, tallies = {}, {}
    order = [(c, sz) for c in range(2) for sz in range(4)]

    def tally(side):
        top = jnp.broadcast_to(tops[side], (8, half_lanes))
        wanted = jnp.concatenate(
            [rolled[pl.ds(lax.rem(z + sz + 3, 4) * 2 + (1 - core if c else core), 1), :]
             for c, sz in order if c == side], axis=1)
        row = lax.broadcasted_iota(jnp.int32, (8, half_lanes), 0)
        offset = jnp.broadcast_to(wanted, (8, half_lanes)) - row
        total = picked = jnp.zeros((8, half_lanes), jnp.float32)
        for first in range(0, logits.shape[0], 8):
            v = logits[pl.ds(first, 8), pl.ds(side * half_lanes, half_lanes)]
            total = total + jnp.exp(v - top)
            picked = picked + jnp.where(offset == first, v, 0.0)
        return jnp.sum(total, axis=0, keepdims=True), jnp.sum(picked, axis=0, keepdims=True)

    def multiply(side, k):
        cols = [cols_of(k, r) for r in live(k)]
        a = jnp.concatenate([weights[:, c] for c in cols], axis=1)
        b = jnp.concatenate([blocks[side, :, :, :, :, c].reshape(half_lanes, c.size) for c in cols], axis=1)
        product = lax.dot_general(a, b, (((1,), (1,)), ((), ())), preferred_element_type=jnp.float32)
        where = (pl.ds(0, vocab), pl.ds(side * half_lanes, half_lanes))
        if k == 0:
            logits[where] = product
        else:
            product = logits[where] + product
            logits[where] = product
        if k == FINAL[side]:
            tops[side] = jnp.max(product, axis=0, keepdims=True)

    for step in (1, -1, 2):
        for r in RS:
            ring(r, 0, (1, 1, 1), (1, 1, 1), cols_of(0, r), ONE, (step,))
    for step in (1, -1, 2):
        for r in RS:
            rest = pl.ds(START[1][r] * UNIT, (TOTAL[r] - STAGES[0][r]) * UNIT)
            ring(r, 0, (1, 1, 1), (1, 1, 1), rest, ONE_REST, (step,))

    logits[pl.ds(vocab, 4), :] = jnp.full((4, logits.shape[1]), -jnp.inf, jnp.float32)
    fetch.wait()
    lane = lax.broadcasted_iota(jnp.int32, (8, 128), 1)
    y0, x0 = lax.rem(y + 3, 4), lax.rem(x + 3, 4)
    turned = pltpu.roll(ids[...], lax.rem(128 - y0 * 32, 128), 1)
    near = pltpu.roll(turned, lax.rem(128 - x0 * 8, 128), 1)
    far = pltpu.roll(turned, lax.rem(160 - x0 * 8, 128), 1)
    turned = jnp.where(lax.rem(lane, 32) + x0 * 8 < 32, near, far) - (replica * 16 + tp) * vocab
    rolled[...] = jnp.where((turned >= 0) & (turned < vocab), turned, -1)

    def other(k):
        shared(k)
        multiply(1, k)
        if k == FINAL[1]:
            tallies[0] = tally(0)

    def rest():
        arrived(ONE_REST)

    def loaded():
        load.wait()

    steps = {"S": second, "G": onward, "T": third, "A": arrive, "F": finish, "M": lambda k: multiply(0, k), "N": other}
    arrived(ONE)
    for step in ORDER:
        if step == "rest":
            arrived(ONE_REST)
        elif step == "load":
            load.wait()
        else:
            steps[step[0]](int(step[1:]))

    tallies[1] = tally(1)
    top, total, picked = [
        jnp.concatenate(both, axis=1)
        for both in ((tops[0], tops[1]), (tallies[0][0], tallies[1][0]), (tallies[0][1], tallies[1][1]))]

    for k in range(8):
        part = slice(128 * k, 128 * k + 128)
        chip[k, 0:1, :] = top[:, part]
        chip[k, 1:2, :] = total[:, part]
        chip[k, 2:3, :] = picked[:, part]
    for k, (c, sz) in enumerate(order):
        dz = (sz - 1) % 4
        if c or dz:
            remote(chip.at[k], chip_in.at[c * 4 + (-dz) % 4], device(dz, 0, 0, c), CHIP).start()
    remote(chip_in.at[pl.ds(1, 7)], chip_in.at[pl.ds(1, 7)], sibling, CHIP).wait_recv()

    def merge(parts):
        best = functools.reduce(jnp.maximum, [p[0] for p in parts])
        total = sum(p[1] * jnp.exp(p[0] - best) for p in parts)
        return best, total, sum(p[2] for p in parts)

    def three_rows(ref, *at):
        return tuple(ref[at + (pl.ds(k, 1), slice(None))] for k in range(3))

    best, total, picked = merge([three_rows(chip, 1)] + [three_rows(chip_in, k) for k in range(1, 8)])
    plane[0:1, :] = best
    plane[1:2, :] = total
    plane[2:3, :] = picked
    for dy in range(4):
        for dx in range(4):
            if dy or dx:
                remote(plane, plane_in.at[(-dy) % 4 * 4 + (-dx) % 4], device(0, dy, dx, False), PLANE).start()
    remote(plane_in.at[pl.ds(1, 15)], plane_in.at[pl.ds(1, 15)], sibling, PLANE).wait_recv()
    group = lax.broadcasted_iota(jnp.int32, (1, 128), 1) // 8
    for sy in range(4):
        for sx in range(4):
            if sy or sx:
                mine = group == (1 - sy) % 4 * 4 + (1 - sx) % 4
                b, t, p = three_rows(plane_in, sy * 4 + sx)
                best, total, picked = jnp.where(mine, b, best), jnp.where(mine, t, total), jnp.where(mine, p, picked)
    final = best
    for shift in (8, 16, 32, 64):
        final = jnp.maximum(final, pltpu.roll(final, shift, 1))
    total = total * jnp.exp(best - final)
    for shift in (8, 16, 32, 64):
        total = total + pltpu.roll(total, shift, 1)
        picked = picked + pltpu.roll(picked, shift, 1)
    out[...] = (picked - final - jnp.log(total))[:, :8]

    drained()
    remote(chip_in.at[pl.ds(1, 7)], chip_in.at[pl.ds(1, 7)], sibling, CHIP).wait_send()
    remote(plane_in.at[pl.ds(1, 15)], plane_in.at[pl.ds(1, 15)], sibling, PLANE).wait_send()


def shards(hidden, head, token_ids):
    vocab, depth = head.shape
    lanes = token_ids.shape[0]
    out = pl.pallas_call(
        kernel,
        out_shape=jax.ShapeDtypeStruct((1, 8), jnp.float32),
        in_specs=[pl.BlockSpec(memory_space=pl.ANY)] * 3,
        out_specs=pl.BlockSpec(memory_space=pltpu.VMEM),
        scratch_shapes=[
            pltpu.VMEM((2, 4, 4, 4, 8, depth), jnp.bfloat16),
            pltpu.VMEM((vocab, depth), jnp.bfloat16),
            pltpu.VMEM((vocab + 4, lanes), jnp.float32),
            pltpu.VMEM((8, 128), jnp.int32),
            pltpu.VMEM((8, 128), jnp.int32),
            pltpu.VMEM((8, 8, 128), jnp.float32),
            pltpu.VMEM((8, 8, 128), jnp.float32),
            pltpu.VMEM((8, 128), jnp.float32),
            pltpu.VMEM((16, 8, 128), jnp.float32),
            pltpu.SemaphoreType.DMA,
            pltpu.SemaphoreType.DMA,
            pltpu.SemaphoreType.DMA,
            pltpu.SemaphoreType.DMA((KINDS + 4,)),
            pltpu.SemaphoreType.DMA((LATE + 4,)),
        ],
        compiler_params=pltpu.CompilerParams(
            collective_id=0, has_side_effects=True, vmem_limit_bytes=60 * 1024 * 1024),
        name="logprob",
    )(hidden, head, token_ids.reshape(8, 128))
    return out.reshape(8)


def solution(mesh):
    in_specs = (P(("replica", "tp"), None), P(("replica", "tp"), None), P())
    out_specs = P(("replica", "tp"))
    return jax.shard_map(shards, mesh=mesh, in_specs=in_specs, out_specs=out_specs, check_vma=False)
```
